32 devices in a mesh: row: 8 (over z, x), col: 4 (over y, core).
Axes of the slice: x: 2, y: 2, z: 4, core: 2. Of those that a mesh axis runs over, the one named last changes fastest.
Arguments:
- sparse_blocks: float32 [4096, 128, 128], P(('row', 'col')), may hold values from -0.5 to 0.5
- panel_rows: float32 [262144, 128], P(('row', 'col')), may hold values from -6 to 6
- block_row: int32 [4096], P(('row', 'col')), may hold values from 0 to 63
- block_owner: int32 [4096, 1], P(('row', 'col')), may hold values from 0 to 31; in each aligned block of 128 rows (0 to 127, 128 to 255, ...) at most 8 rows name the same one
- block_offset: int32 [4096], P(('row', 'col')), may hold values from 0 to 63
Outputs:
- result: float32 [262144, 128], P(('row', 'col'))
The draws below stay inside these ranges and needn't reach their ends.
Inputs may be any that keep to these rules, and one draw needn't show every extreme that they name: `block_owner`: among the blocks of one device, at most 8 name the same owner, a bound that some block reaches.
All inputs are finite; a program needn't handle non-finite values.
Results may differ from the reference program's by a relative error of at most 0.0001.
Values sent between devices are 32-bit elements; how exact they have to be, the bound alone decides.
A program may use at most 192 MiB of HBM per device.

```python
import math
import jax
import jax.numpy as jnp
import numpy as np
from jax import lax

BLK = 128
PANEL = 128
RB_DEV = 64
SLOTS = 128
CAP = 8
NB = 2048
NNZ = 4096
N_ROW = 8
N_COL = 4


def plant(array, rng, smallest, top_value):
    index_at = [jax.random.randint(jax.random.fold_in(rng, axis), (), 0, length) for axis, length in enumerate(array.shape)]
    widest = array.shape.index(max(array.shape))
    beside = index_at[:widest] + [(index_at[widest] + 1) % array.shape[widest]] + index_at[widest + 1:]
    return array.at[tuple(index_at)].set(smallest).at[tuple(beside)].set(top_value)


def steps_of(key, shape, pieces, low, top_value):
    gain, own = 1.0, jax.random.fold_in(key, 6)
    for position, shards_of in pieces:
        draws = jnp.exp(jax.random.uniform(jax.random.fold_in(own, position), (shards_of,), jnp.float32, low / len(pieces), top_value / len(pieces)))
        gain = gain * jnp.repeat(draws, shape[position] // shards_of).reshape([-1 if axis == position else 1 for axis in range(len(shape))])
    return gain


def rank_table(number_of, lean):
    weights = [(1 << 20) // math.isqrt(rank ** lean) + 1 for rank in range(1, number_of + 1)]
    scale = 1 + sum(weights) // (1 << 30)
    return np.cumsum(np.array([max(1, weight // scale) for weight in weights]))


def ranked_ids(stream_key, extent, count, slope):
    listing = rank_table(count, slope)
    ticket = jax.random.randint(jax.random.fold_in(stream_key, 1), extent, 0, int(listing[count - 1]))
    standing = jnp.searchsorted(jnp.asarray(listing, jnp.int32), ticket, side="right")
    return jax.random.permutation(jax.random.fold_in(stream_key, 2), count)[standing].astype(jnp.int32)


def deal_out(stream_key, own, number, rows, number_of, top, limit, skew):
    sequence = jax.random.permutation(stream_key, number_of)
    heavy_load, common = shares(number_of, rows * top, limit, skew, True), shares(number_of, rows * top, limit, skew, False)
    places = jnp.arange(number_of)

    def named(lengths, offset_by):
        used = int((lengths > 0).sum())
        fixed = max(1, used // 4)
        moved = fixed + (places - fixed + offset_by * (used - fixed)) % max(1, number_of - fixed)
        return jnp.zeros((number_of,), jnp.int32).at[sequence[jnp.where(places < fixed, places, moved)]].set(jnp.asarray(lengths, jnp.int32))

    lengths = jnp.where(number % 4 == 0, named(heavy_load, number // 4), named(common, number - number // 4 - 1))
    mixed = jax.random.permutation(jax.random.fold_in(own, 3), number_of)
    source_of, sink = mixed[0:number_of // 2 * 2:2], mixed[1:number_of // 2 * 2:2]
    slack = jnp.minimum(lengths[source_of] - 1, limit - lengths[sink]) // 2
    slack = jnp.where((source_of == sequence[0]) | (sink == sequence[0]) | (lengths[sink] == 0), 0, jnp.maximum(slack, 0))
    moved = jax.random.randint(jax.random.fold_in(own, 4), (number_of // 2,), 0, 1 << 20) % (slack + 1)
    lengths = lengths.at[source_of].add(-moved).at[sink].add(moved)
    items = jnp.searchsorted(jnp.cumsum(lengths), jnp.arange(rows * top), side="right").astype(jnp.int32)
    table = items.reshape(top, rows).T
    table = table[jax.random.permutation(jax.random.fold_in(own, 1), rows)]
    offset_by = jax.random.randint(jax.random.fold_in(own, 2), (rows, 1), 0, top)
    return jnp.take_along_axis(table, (jnp.arange(top)[None, :] + offset_by) % top, axis=1)


def shares(number_of, total, limit, lean, full):
    loads = [(1 << 20) // math.isqrt(rank ** lean) + 1 for rank in range(1, number_of + 1)]
    largest = limit if full else min(limit, max(-(-total // number_of), total * loads[0] // sum(loads)))
    least = 1 if total - largest >= number_of - 1 else 0
    given, surplus = [largest] + [least] * (number_of - 1), total - largest - least * (number_of - 1)
    while surplus > 0:
        movable = [i for i in range(1, number_of) if given[i] < largest] or [i for i in range(1, number_of) if given[i] < limit]
        pool, remaining = sum([loads[i] for i in movable]), surplus
        for i in movable:
            more = min(limit - given[i], max(1, remaining * loads[i] // pool), surplus)
            given[i] = given[i] + more
            surplus = surplus - more
    return np.array(given)


def noise(rng, dims, deviation, reach, pieces=(), kind=jnp.bfloat16):
    values = deviation * jax.random.normal(rng, dims, jnp.float32)
    if pieces:
        values = values * steps_of(rng, dims, pieces, -0.22, 0.18)
    return jnp.clip(values, -reach, reach).astype(kind)


def setup_inputs(seed: int = 0) -> dict:
    keys = jax.random.split(jax.random.key(seed), 6)
    sparse_blocks = noise(keys[0], (NNZ, BLK, BLK), BLK ** -0.5, 0.5, ((0, 32),), jnp.float32)
    panel_rows = noise(keys[1], (NB * BLK, PANEL), 1.0, 6.0, ((0, 32),), jnp.float32)
    block_row = plant(ranked_ids(keys[2], (NNZ,), RB_DEV, 2), jax.random.fold_in(keys[2], 3), 0, RB_DEV - 1).astype(jnp.int32)
    block_owner_keys = jax.random.split(jax.random.fold_in(keys[3], 1), NNZ // SLOTS)
    block_owner_turns = jax.random.permutation(jax.random.fold_in(keys[3], 3), NNZ // SLOTS)
    block_owner = jax.vmap(lambda own, number: deal_out(jax.random.fold_in(keys[3], 2), own, number, SLOTS, N_ROW * N_COL, 1, CAP, 2))(block_owner_keys, block_owner_turns).reshape((NNZ, 1))
    block_offset = plant(jax.random.randint(keys[4], (NNZ,), 0, RB_DEV), jax.random.fold_in(keys[4], 1), 0, RB_DEV - 1).astype(jnp.int32)
    return {"sparse_blocks": sparse_blocks, "panel_rows": panel_rows, "block_row": block_row, "block_owner": block_owner, "block_offset": block_offset}


def reference(sparse_blocks, panel_rows, block_row, block_owner, block_offset):
    device_count = N_ROW * N_COL
    panel_blocks = panel_rows.reshape(device_count * RB_DEV, BLK, PANEL)
    owners = block_owner[:, 0]

    def advance(device_index, accum):
        device_index = device_index.astype(jnp.int32)
        start = device_index * SLOTS
        piece_a = lax.dynamic_slice_in_dim(sparse_blocks, start, SLOTS, 0)
        row_ids = (lax.dynamic_slice_in_dim(block_row, start, SLOTS, 0) + device_index * RB_DEV).astype(jnp.int32)
        col_ids = (lax.dynamic_slice_in_dim(owners, start, SLOTS, 0) * RB_DEV + lax.dynamic_slice_in_dim(block_offset, start, SLOTS, 0)).astype(jnp.int32)
        products = jnp.einsum("sij,sik->sjk", piece_a, panel_blocks[row_ids], precision=lax.Precision.HIGHEST)
        return accum.at[col_ids].add(products)

    accum = lax.fori_loop(0, device_count, advance, jnp.zeros((device_count * RB_DEV, BLK, PANEL), jnp.float32))
    return accum.reshape(device_count * RB_DEV * BLK, PANEL)
```

```python
import functools

import jax
import jax.numpy as jnp
from jax import lax
from jax.experimental import pallas as pl
from jax.experimental.pallas import tpu as pltpu
from jax.sharding import PartitionSpec as P

AXES = ("row", "col")
VMEM_LIMIT = 60 * 1024 * 1024


def split_parts(value):
    high = value.astype(jnp.bfloat16)
    low = (value - high.astype(jnp.float32)).astype(jnp.bfloat16)
    return high, low


def block_product(block, panel):
    block_high, block_low = split_parts(block)
    panel_high, panel_low = split_parts(panel)
    dims = (((0,), (0,)), ((), ()))
    dot = functools.partial(lax.dot_general, dimension_numbers=dims, preferred_element_type=jnp.float32)
    return dot(
        jnp.concatenate([block_high, block_low], axis=0),
        jnp.concatenate([panel_high, panel_high], axis=0),
    ) + dot(block_high, panel_low)


def product_kernel(group, source_ref, row_ref, sparse_ref, panel_ref, out_ref):
    step = pl.program_id(0)
    for k in range(group):
        source = source_ref[step * group + k]

        @pl.when(source >= 0)
        def _():
            row = row_ref[jnp.maximum(source, 0)]
            out_ref[k] = block_product(sparse_ref[jnp.maximum(source, 0)], panel_ref[row])

        @pl.when(source < 0)
        def _():
            out_ref[k] = jnp.zeros(out_ref.shape[1:], jnp.float32)


def send_products(source, block_row, sparse_blocks, panel_blocks):
    slots = source.shape[0]
    count, size, _ = sparse_blocks.shape
    local_blocks, _, width = panel_blocks.shape
    group = min(8, slots)
    whole = lambda step, *_: (0, 0, 0)
    return pl.pallas_call(
        functools.partial(product_kernel, group),
        grid_spec=pltpu.PrefetchScalarGridSpec(
            num_scalar_prefetch=2,
            grid=(slots // group,),
            in_specs=[
                pl.BlockSpec((count, size, size), whole),
                pl.BlockSpec((local_blocks, size, width), whole),
            ],
            out_specs=pl.BlockSpec((group, size, width), lambda step, *_: (step, 0, 0)),
        ),
        out_shape=jax.ShapeDtypeStruct((slots, size, width), jnp.float32),
        compiler_params=pltpu.CompilerParams(vmem_limit_bytes=VMEM_LIMIT),
        cost_estimate=pl.CostEstimate(
            flops=6 * slots * size * size * width,
            bytes_accessed=4 * (count * size * size + (local_blocks + slots) * size * width),
            transcendentals=0,
        ),
    )(source, block_row, sparse_blocks, panel_blocks)


def collect_kernel(group, label_ref, arrived_ref, out_ref):
    step = pl.program_id(0)

    @pl.when(step == 0)
    def _():
        out_ref[...] = jnp.zeros(out_ref.shape, jnp.float32)

    for k in range(group):
        label = label_ref[step * group + k]

        @pl.when(label >= 0)
        def _():
            out_ref[jnp.maximum(label, 0)] += arrived_ref[k]


def collect(labels, arrived, local_blocks):
    slots, size, width = arrived.shape
    group = min(8, slots)
    return pl.pallas_call(
        functools.partial(collect_kernel, group),
        grid_spec=pltpu.PrefetchScalarGridSpec(
            num_scalar_prefetch=1,
            grid=(slots // group,),
            in_specs=[pl.BlockSpec((group, size, width), lambda step, *_: (step, 0, 0))],
            out_specs=pl.BlockSpec((local_blocks, size, width), lambda step, *_: (0, 0, 0)),
        ),
        out_shape=jax.ShapeDtypeStruct((local_blocks, size, width), jnp.float32),
        compiler_params=pltpu.CompilerParams(vmem_limit_bytes=VMEM_LIMIT),
        cost_estimate=pl.CostEstimate(
            flops=slots * size * width,
            bytes_accessed=4 * (slots + local_blocks) * size * width,
            transcendentals=0,
        ),
    )(labels, arrived)


def body(sparse_blocks, panel_rows, block_row, block_owner, block_offset):
    device_count = lax.axis_size("row") * lax.axis_size("col")
    half_count = device_count // 2
    slot_count, size, _ = sparse_blocks.shape
    width = panel_rows.shape[1]
    local_blocks = panel_rows.shape[0] // size
    per_owner = max(2, 2 * slot_count // device_count)
    half_slots = half_count * per_owner
    me = lax.axis_index(AXES)
    my_half = me // half_count
    groups = [list(range(half_count)), list(range(half_count, device_count))]
    exchange = functools.partial(
        lax.all_to_all, axis_name=AXES, split_axis=0, concat_axis=0, tiled=True, axis_index_groups=groups
    )

    owner = block_owner[:, 0]
    index = jnp.arange(slot_count, dtype=jnp.int32)
    earlier = (owner[:, None] == owner[None, :]) & (index[None, :] < index[:, None])
    order = jnp.sum(earlier.astype(jnp.int32), axis=1)
    half_of = (owner // half_count != my_half).astype(jnp.int32)
    position = half_of * half_slots + (owner % half_count) * per_owner + order
    hit = position[None, :] == jnp.arange(2 * half_slots, dtype=jnp.int32)[:, None]
    source = jnp.max(jnp.where(hit, index[None, :], -1), axis=1)
    label = jnp.max(jnp.where(hit, block_offset[None, :], -1), axis=1).astype(jnp.float32)
    near_source, far_source = source[:half_slots], source[half_slots:]
    label = label.reshape(2, half_count, per_owner).transpose(1, 0, 2).reshape(half_count, 2 * per_owner)
    labels = exchange(label).reshape(half_count, 2, per_owner).astype(jnp.int32)
    near_labels = labels[:, 0].reshape(half_slots)
    far_labels = labels[:, 1].reshape(half_slots)

    panel_blocks = panel_rows.reshape(local_blocks, size, width)
    far_products = send_products(far_source, block_row, sparse_blocks, panel_blocks)
    far_arrived = exchange(far_products)
    near_products = send_products(near_source, block_row, sparse_blocks, panel_blocks)
    far_sums = collect(far_labels, far_arrived, local_blocks)
    far_sums, near_products = lax.optimization_barrier((far_sums, near_products))
    across = [(d, (d + half_count) % device_count) for d in range(device_count)]
    crossed = lax.ppermute(far_sums, AXES, across)
    near_arrived = exchange(near_products)
    near_sums = collect(near_labels, near_arrived, local_blocks)
    return (near_sums + crossed).reshape(local_blocks * size, width)


def solution(mesh):
    placed = (
        P(AXES, None, None),
        P(AXES, None),
        P(AXES),
        P(AXES, None),
        P(AXES),
    )
    return jax.shard_map(
        body, mesh=mesh, in_specs=placed, out_specs=P(AXES, None), check_vma=False
    )
```
